32 devices in a mesh: ka: 2 (over x), band: 16 (over z, y, core).
Axes of the slice: x: 2, y: 2, z: 4, core: 2. Of those that a mesh axis runs over, the one named last changes fastest.
Arguments:
- psi_hat: float32 [2, 12, 2, 128, 128, 128], P('ka', None, None, 'band'), may hold values from -1.5 to 1.5
- occupations: int32 [2, 12], P('ka'), may hold values from 0 to 2
- weights: int32 [2], P('ka'), may hold values from 1 to 6
- density_in: float32 [128, 128, 128], P('band'), may hold values from -12 to 12
- dens_hist: float32 [8, 128, 128, 128], P(None, 'band'), may hold values from -3 to 3
- resid_hist: float32 [8, 128, 128, 128], P(None, 'band'), may hold values from -12 to 12
Outputs:
- out_density: float32 [128, 128, 128], P('band')
- mixed_density: float32 [128, 128, 128], P('band')
The draws below stay inside these ranges and needn't reach their ends.
All inputs are finite; a program needn't handle non-finite values.
Results may differ from the reference program's by a relative error of at most 0.0003.
Values sent between devices are 32-bit elements; how exact they have to be, the bound alone decides.
A program may use at most 128 MiB of HBM per device.

```python
from functools import partial
import jax
import jax.numpy as jnp
from jax import lax

NG = 128
BANDS = 12
HIST = 8
KPTS = 2


def common_field(key):
    return jax.random.truncated_normal(jax.random.fold_in(key, 7), -5.0, 5.0, (NG, NG, NG), jnp.float32)


def draw_density_in(key, part):
    shared = common_field(key)
    noise_part = jax.random.truncated_normal(jax.random.fold_in(key, 11), -5.0, 5.0, (NG, NG, NG), jnp.float32)
    return shared + 0.3 * noise_part


def draw_resid_hist(key, part):
    shared = common_field(key)
    loadings = jax.random.uniform(jax.random.fold_in(key, 13), (HIST, 1, 1, 1), jnp.float32, -1.0, 1.0)
    noise_part = jax.random.truncated_normal(jax.random.fold_in(key, 17), -5.0, 5.0, (HIST, NG, NG, NG), jnp.float32)
    return loadings * shared + 0.5 * noise_part


def touch_ends(array, stream_key, least, largest):
    longest = array.shape.index(max(array.shape))
    spots = []
    for shift in (0, 1):
        where = [jax.random.randint(jax.random.fold_in(stream_key, axis), (), 0, length) for axis, length in enumerate(array.shape)]
        where[longest] = (where[longest] + shift) % array.shape[longest]
        spots.append(tuple(where))
    return array.at[spots[0]].set(least).at[spots[1]].set(largest)


def level_of(stream_key, dims, split, smallest, top_value):
    level = 1.0
    for dim, parts in split:
        heights = jax.random.uniform(jax.random.fold_in(jax.random.fold_in(stream_key, 6), dim), (parts,), jnp.float32, smallest / len(split), top_value / len(split))
        level = level * jnp.repeat(jnp.exp(heights), dims[dim] // parts).reshape((-1,) + (1,) * (len(dims) - 1 - dim))
    return level


def gaussian(stream_key, shape, deviation, most, cuts=(), kind=jnp.bfloat16):
    gain = level_of(stream_key, shape, cuts, -0.22, 0.18) if cuts else 1.0
    result = jax.random.normal(stream_key, shape, jnp.float32) * deviation * gain
    return jnp.minimum(jnp.maximum(result, -most), most).astype(kind)


def setup_inputs(seed: int = 0) -> dict:
    key_list = jax.random.split(jax.random.key(seed), 7)
    psi_hat = gaussian(key_list[0], (KPTS, BANDS, 2, NG, NG, NG), 0.25, 1.5, ((0, 2), (3, 16)), jnp.float32)
    occupations = touch_ends(jax.random.randint(key_list[1], (KPTS, BANDS), 0, 3), jax.random.fold_in(key_list[1], 1), 0, 2).astype(jnp.int32)
    weights = jax.random.randint(key_list[2], (KPTS,), 1, 7).astype(jnp.int32)
    density_in = draw_density_in(jax.random.fold_in(key_list[6], 71), 0)
    dens_hist = gaussian(key_list[4], (HIST, NG, NG, NG), 0.5, 3.0, ((1, 16),), jnp.float32)
    resid_hist = draw_resid_hist(jax.random.fold_in(key_list[6], 71), 0)
    return dict(psi_hat=psi_hat, occupations=occupations, weights=weights, density_in=density_in, dens_hist=dens_hist, resid_hist=resid_hist)


highest = lax.Precision.HIGHEST
beta_mix = 0.3
regular = 0.01

def dft_tables():
    indices = jnp.arange(NG, dtype=jnp.int32)
    product = indices[:, None] * indices[None, :] % NG
    angles = product.astype(jnp.float32) * jnp.float32(2.0 * 3.141592653589793 / NG)
    return (jnp.cos(angles), jnp.sin(angles))

def rotate(pattern, real_part, imag_part, cosine_table, sine_table):
    einsum = partial(jnp.einsum, precision=highest)
    out_real = einsum(pattern, real_part, cosine_table) - einsum(pattern, imag_part, sine_table)
    out_imag = einsum(pattern, real_part, sine_table) + einsum(pattern, imag_part, cosine_table)
    return (out_real, out_imag)

def band_power(coeffs, cosine_table, sine_table):
    real_part, imag_part = rotate('pqk,kz->zpq', coeffs[0], coeffs[1], cosine_table, sine_table)
    real_part, imag_part = rotate('zpq,qy->zpy', real_part, imag_part, cosine_table, sine_table)
    real_part, imag_part = rotate('zpy,px->zxy', real_part, imag_part, cosine_table, sine_table)
    return (real_part * real_part + imag_part * imag_part) * jnp.float32(1.0 / NG ** 3)

def broyden(density, density_in, dens_hist, resid_hist):
    residual_now = density - density_in
    gram = jnp.einsum('hzxy,gzxy->hg', resid_hist, resid_hist, precision=highest)
    projections = jnp.einsum('hzxy,zxy->h', resid_hist, residual_now, precision=highest)
    system = gram + regular * jnp.diag(jnp.diag(gram))
    chol_factor = jnp.linalg.cholesky(system)
    mix_coefs = jax.scipy.linalg.cho_solve((chol_factor, True), projections)
    update = jnp.einsum('h,hzxy->zxy', mix_coefs, dens_hist + beta_mix * resid_hist, precision=highest)
    return density_in + beta_mix * residual_now - update

def reference(psi_hat, occupations, weights, density_in, dens_hist, resid_hist):
    cosine_table, sine_table = dft_tables()
    weight_total = jnp.sum(weights.astype(jnp.float32))

    def per_point(point_total, point_inputs):
        coeffs_point, occ_point, weight_point = point_inputs

        def per_band(band_total, band_inputs):
            coeffs_band, occ_band = band_inputs
            power = band_power(coeffs_band, cosine_table, sine_table)
            return (band_total + occ_band.astype(jnp.float32) * power, None)
        pool_term, unused = lax.scan(per_band, jnp.zeros((NG, NG, NG), jnp.float32), (coeffs_point, occ_point))
        return (point_total + pool_term * (weight_point.astype(jnp.float32) / weight_total), None)
    density, unused = lax.scan(per_point, jnp.zeros((NG, NG, NG), jnp.float32), (psi_hat, occupations, weights))
    mixed_density = broyden(density, density_in, dens_hist, resid_hist)
    return (density, mixed_density)
```

```python
from functools import partial

import jax
import jax.numpy as jnp
import numpy as np
from jax import lax
from jax.experimental import pallas as pl
from jax.experimental.pallas import tpu as pltpu
from jax.sharding import PartitionSpec as P

beta_mix = 0.3
regular = 0.01
LAG = 3
MESH = pl.DeviceIdType.MESH


def rotation_tables(size):
    indices = np.arange(size)
    angles = (indices[:, None] * indices[None, :] % size) * (2.0 * np.pi / size)
    cosine, sine = np.cos(angles), np.sin(angles)
    table = np.block([[cosine, sine], [-sine, cosine]]).astype(np.float32)
    high = table.astype(jnp.bfloat16)
    low = (table - high.astype(np.float32)).astype(jnp.bfloat16)
    return np.stack([high, low, high.T, low.T])


def split(value):
    high = value.astype(jnp.bfloat16)
    return high, (value - high.astype(jnp.float32)).astype(jnp.bfloat16)


def dot3(left, right, contract):
    dims = (contract, ((), ()))
    dot = partial(lax.dot_general, dimension_numbers=dims, preferred_element_type=jnp.float32)
    return dot(left[0], right[0]) + (dot(left[0], right[1]) + dot(left[1], right[0]))


def partner(index, step, count):
    if count & (count - 1):
        return lax.rem(index + step, count)
    result, bit = index, 1
    while bit < count:
        if step & bit:
            result = result + bit * (1 - 2 * lax.rem(index // bit, 2))
        bit *= 2
    return result


def total(value):
    return jnp.sum(jnp.sum(value, axis=0, keepdims=True), axis=1, keepdims=True)


def step_kernel(
    occ_ref, weight_ref, tables_hbm, psi_hbm, density_in_hbm, dens_hbm, resid_hbm,
    density_hbm, mixed_hbm,
    tables, psi, send, recv, pools, resid, dens, density_in, mixed, share, wbuf, grams, lates,
    late_acc, inverse,
    in_sem, psi_sem, send_sem, recv_sem, small_send, small_recv, pool_send, pool_recv, out_sem,
):
    points, devices = lax.axis_size("ka"), lax.axis_size("band")
    bands, _, depth, _, planes, size = send.shape[0], *send.shape[1:]
    hist = resid.shape[0]
    everyone = points * devices
    pairs = depth // 2
    ka, me = lax.axis_index("ka"), lax.axis_index("band")
    flat = ka * devices + me
    steps = range(devices - 1, 0, -1)
    some_band = (ka, partner(me, 1, devices))
    some_point = (lax.rem(ka + 1, points), me)

    def remote(source, target, send_s, recv_s, device):
        return pltpu.make_async_remote_copy(
            src_ref=source, dst_ref=target, send_sem=send_s, recv_sem=recv_s,
            device_id=device, device_id_type=MESH,
        )

    def psi_copy(band, slot):
        return pltpu.make_async_copy(psi_hbm.at[0, band], psi.at[slot], psi_sem.at[slot])

    tables_copy = pltpu.make_async_copy(tables_hbm, tables, in_sem.at[0])
    resid_copy = pltpu.make_async_copy(resid_hbm, resid, in_sem.at[1])
    dens_copy = pltpu.make_async_copy(dens_hbm, dens, in_sem.at[2])
    base_copy = pltpu.make_async_copy(density_in_hbm, density_in, in_sem.at[3])

    psi_copy(0, 0).start()
    tables_copy.start()
    psi_copy(1, 1).start()
    barrier = pltpu.get_barrier_semaphore()

    def greet(step, carry):
        other = lax.rem(flat + step, everyone)
        pl.semaphore_signal(
            barrier, inc=1, device_id=(other // devices, lax.rem(other, devices)),
            device_id_type=MESH,
        )
        return carry

    lax.fori_loop(1, everyone, greet, 0)
    base_copy.start()
    resid_copy.start()
    dens_copy.start()
    pools[pl.ds(ka, 1)] = jnp.zeros((1, depth, size, size), jnp.float32)
    late_acc[...] = jnp.zeros(late_acc.shape, jnp.float32)
    wbuf[pl.ds(ka, 1)] = jnp.full((1, 1, 128), weight_ref[0].astype(jnp.float32))
    tables_copy.wait()

    def produce(band, slot):
        psi_copy(band, slot).wait()
        for p in range(planes):
            pair = jnp.concatenate([psi[slot, 0, p], psi[slot, 1, p]], axis=1)
            after_kz = dot3((tables[2], tables[3]), split(pair), ((1,), (1,)))
            rows = jnp.concatenate([after_kz[:size], after_kz[size:]], axis=1)
            after_ky = dot3(split(rows), (tables[0], tables[1]), ((1,), (0,)))
            for part in range(2):
                piece = after_ky[:, part * size : (part + 1) * size]
                send[band, :, :, part, p, :] = piece.reshape(devices, depth, size)
        recv[band, pl.ds(me, 1)] = send[band, pl.ds(me, 1)]

    def transform(band, pair):
        columns = []
        for near in range(2):
            z = 2 * pair + near
            parts = [recv[band, :, z, c].reshape(devices * planes, size) for c in range(2)]
            columns.append(jnp.concatenate(parts, axis=0))
        field = dot3(
            (tables[2], tables[3]), split(jnp.concatenate(columns, axis=1)), ((1,), (0,))
        )
        power = field[:size] * field[:size] + field[size:] * field[size:]
        scale = share[...] * occ_ref[0, band].astype(jnp.float32)
        for near in range(2):
            pools[ka, 2 * pair + near] += scale * power[:, near * size : (near + 1) * size]

    def consume(band):
        remote(
            send.at[band, pl.ds(0, devices - 1)], recv.at[band, pl.ds(0, devices - 1)],
            send_sem.at[band], recv_sem.at[band], some_band,
        ).wait_recv()

        def body(pair, carry):
            transform(band, pair)
            return carry

        lax.fori_loop(0, pairs, body, 0)

    def send_weight():
        for step in range(1, points):
            remote(
                wbuf.at[ka], wbuf.at[ka], small_send.at[0], small_recv.at[0],
                (lax.rem(ka + step, points), me),
            ).start()

    def history():
        remote(
            wbuf.at[pl.ds(0, points - 1)], wbuf.at[pl.ds(0, points - 1)],
            small_send.at[0], small_recv.at[0], some_point,
        ).wait()
        weight_total = wbuf[0]
        for k in range(1, points):
            weight_total = weight_total + wbuf[k]
        share[...] = wbuf[ka] / weight_total * jnp.float32(1.0 / size**3)
        base_copy.wait()
        resid_copy.wait()
        dens_copy.wait()
        which = [(h, g) for h in range(hist) for g in range(h + 1)]
        blocks = size // 8

        def body(i, sums):
            z, x = i // blocks, pl.multiple_of(lax.rem(i, blocks) * 8, 8)
            rows = [resid[h, z, pl.ds(x, 8)] for h in range(hist)]
            start = density_in[z, pl.ds(x, 8)]
            for h in range(hist):
                dens[h, z, pl.ds(x, 8)] = dens[h, z, pl.ds(x, 8)] + beta_mix * rows[h]
            products = [rows[h] * rows[g] for h, g in which] + [row * start for row in rows]
            return tuple(s + p for s, p in zip(sums, products))

        zeros = tuple(jnp.zeros((8, size), jnp.float32) for _ in range(len(which) + hist))
        sums = lax.fori_loop(0, depth * blocks, body, zeros)
        lane = lax.broadcasted_iota(jnp.int32, (1, 128), 1)
        row = jnp.zeros((1, 128), jnp.float32)
        for (h, g), value in zip(which, sums):
            here = (lane == h * hist + g) | (lane == g * hist + h)
            row = jnp.where(here, total(value), row)
        for h in range(hist):
            row = jnp.where(lane == hist * hist + h, total(sums[len(which) + h]), row)
        grams[pl.ds(me, 1)] = row[None]
        for step in steps:
            remote(
                grams.at[me], grams.at[me], small_send.at[1], small_recv.at[1],
                (ka, partner(me, step, devices)),
            ).start()

    def factor():
        rest = pl.ds(0, devices - 1)
        remote(
            grams.at[rest], grams.at[rest], small_send.at[1], small_recv.at[1], some_band
        ).wait()
        row = grams[0]
        for d in range(1, devices):
            row = row + grams[d]
        lane = lax.broadcasted_iota(jnp.int32, (hist, 128), 1)
        level = lax.broadcasted_iota(jnp.int32, (hist, 128), 0)
        wide = jnp.broadcast_to(row, (hist, 128))
        start = jnp.zeros((1, 1), jnp.float32)
        gram = jnp.zeros((hist, 128), jnp.float32)
        for g in range(hist):
            picked = jnp.sum(
                jnp.where(lane == level * hist + g, wide, 0.0), axis=1, keepdims=True
            )
            gram = jnp.where(lane == g, picked, gram)
        first = jnp.sum(
            jnp.where(lane == hist * hist + level, wide, 0.0), axis=1, keepdims=True
        )
        start = jnp.sum(jnp.where(lane == level, first, 0.0), axis=0, keepdims=True)
        work = jnp.where(lane == level, gram + regular * gram, gram)
        right = jnp.where(lane == level, jnp.float32(1.0), 0.0)
        for j in range(hist):
            pivot = jnp.sum(
                jnp.where((lane == j) & (level == j), work, 0.0), axis=(0, 1), keepdims=True
            )
            root = jnp.sqrt(pivot)
            column = jnp.sum(jnp.where(lane == j, work, 0.0), axis=1, keepdims=True) / root
            line = jnp.sum(jnp.where(level == j, work, 0.0), axis=0, keepdims=True) / root
            solved = jnp.sum(jnp.where(level == j, right, 0.0), axis=0, keepdims=True) / root
            work = work - column * line
            right = jnp.where(
                level == j, solved, jnp.where(level > j, right - column * solved, right)
            )
        inverse[0:hist] = right
        inverse[hist : hist + 1] = start

    def step(band, carry):
        slot = lax.rem(band, 2)
        produce(band, slot)

        @pl.when(band == 0)
        def _():
            pl.semaphore_wait(barrier, everyone - 1)
            send_weight()

        @pl.when(band < bands - 1)
        def _():
            for s in steps:
                other = partner(me, s, devices)
                remote(
                    send.at[band, other], recv.at[band, me],
                    send_sem.at[band], recv_sem.at[band], (ka, other),
                ).start()

        @pl.when(band == bands - 1)
        def _():
            for pair in range(pairs):
                for s in steps:
                    other = partner(me, s, devices)
                    cut = pl.ds(2 * pair, 2)
                    remote(
                        send.at[bands - 1, other, cut], recv.at[bands - 1, me, cut],
                        send_sem.at[bands - 1 + pair], recv_sem.at[bands - 1 + pair],
                        (ka, other),
                    ).start()

        @pl.when(band + 2 < bands)
        def _():
            psi_copy(band + 2, slot).start()

        @pl.when(band == LAG - 1)
        def _():
            history()

        @pl.when(band >= LAG)
        def _():
            consume(band - LAG)

        return carry

    lax.fori_loop(0, bands, step, 0)
    factor()

    def drain(band, carry):
        consume(band)
        return carry

    lax.fori_loop(bands - LAG, bands - 1, drain, 0)

    def pool_copy(pair, device):
        cut = pl.ds(2 * pair, 2)
        return remote(
            pools.at[ka, cut], pools.at[ka, cut], pool_send.at[pair], pool_recv.at[pair], device
        )

    def pool_wait(pair):
        rest = pools.at[pl.ds(0, points - 1), pl.ds(2 * pair, 2)]
        return remote(rest, rest, pool_send.at[pair], pool_recv.at[pair], some_point)

    def density_out(pair):
        cut = pl.ds(2 * pair, 2)
        return pltpu.make_async_copy(
            mixed.at[0, cut], density_hbm.at[cut], out_sem.at[pair]
        )

    def mixed_out(pair):
        cut = pl.ds(2 * pair, 2)
        return pltpu.make_async_copy(
            mixed.at[1, cut], mixed_hbm.at[cut], out_sem.at[pairs + pair]
        )

    def gather(pair):
        pool_wait(pair).wait()
        for z in (2 * pair, 2 * pair + 1):
            density = pools[0, z]
            for k in range(1, points):
                density = density + pools[k, z]
            start = density_in[z]
            mixed[0, z] = density
            mixed[1, z] = start + beta_mix * (density - start)
        density_out(pair).start()

    for pair in range(pairs):
        cut = pl.ds(2 * pair, 2)
        rest = pl.ds(0, devices - 1)
        remote(
            send.at[bands - 1, rest, cut], recv.at[bands - 1, rest, cut],
            send_sem.at[bands - 1 + pair], recv_sem.at[bands - 1 + pair], some_band,
        ).wait_recv()
        transform(bands - 1, pair)
        for s in range(1, points):
            pool_copy(pair, (lax.rem(ka + s, points), me)).start()
        for h in range(hist):
            value = late_acc[h]
            for z in (2 * pair, 2 * pair + 1):
                product = resid[h, z] * pools[ka, z]
                value = value + jnp.sum(product.reshape(size // 8, 8, size), axis=0)
            late_acc[h] = value
        if pair:
            gather(pair - 1)

    lane = lax.broadcasted_iota(jnp.int32, (hist, 128), 1)
    level = lax.broadcasted_iota(jnp.int32, (hist, 128), 0)
    sums = jnp.sum(jnp.sum(late_acc[...], axis=1), axis=1, keepdims=True)
    row = jnp.sum(jnp.where(lane == level, sums, 0.0), axis=0, keepdims=True)
    lates[pl.ds(flat, 1)] = row[None]

    def tell(step, carry):
        other = lax.rem(flat + step, everyone)
        remote(
            lates.at[flat], lates.at[flat], small_send.at[2], small_recv.at[2],
            (other // devices, lax.rem(other, devices)),
        ).start()
        return carry

    lax.fori_loop(1, everyone, tell, 0)
    gather(pairs - 1)
    rest = lates.at[pl.ds(0, everyone - 1)]
    remote(rest, rest, small_send.at[2], small_recv.at[2], some_band).wait()
    late = lates[0]
    for d in range(1, everyone):
        late = late + lates[d]
    factor_inverse = inverse[0:hist]
    halfway = jnp.sum(
        factor_inverse * (late - inverse[hist : hist + 1]), axis=1, keepdims=True
    )
    coefs = jnp.sum(factor_inverse * halfway, axis=0, keepdims=True)
    coefs = [
        jnp.sum(jnp.where(lane[:1] == h, coefs, 0.0), axis=1, keepdims=True) for h in range(hist)
    ]
    for pair in range(pairs):
        for z in (2 * pair, 2 * pair + 1):
            update = coefs[0] * dens[0, z]
            for h in range(1, hist):
                update = update + coefs[h] * dens[h, z]
            mixed[1, z] = mixed[1, z] - update
        mixed_out(pair).start()

    rest = pl.ds(0, devices - 1)

    def sent(band, carry):
        remote(
            send.at[band, rest], recv.at[band, rest], send_sem.at[band], recv_sem.at[band],
            some_band,
        ).wait_send()
        return carry

    lax.fori_loop(0, bands - 1, sent, 0)
    for pair in range(pairs):
        cut = pl.ds(2 * pair, 2)
        remote(
            send.at[bands - 1, rest, cut], recv.at[bands - 1, rest, cut],
            send_sem.at[bands - 1 + pair], recv_sem.at[bands - 1 + pair], some_band,
        ).wait_send()
        density_out(pair).wait()
        mixed_out(pair).wait()


def shards(psi_hat, occupations, weights, density_in, dens_hist, resid_hist):
    devices, points = lax.axis_size("band"), lax.axis_size("ka")
    _, bands, _, planes, size, _ = psi_hat.shape
    hist = resid_hist.shape[0]
    depth = size // devices
    pairs = depth // 2
    tables = jnp.asarray(rotation_tables(size))
    anywhere = pl.BlockSpec(memory_space=pl.ANY)
    scalars = pl.BlockSpec(memory_space=pltpu.SMEM)
    slab = jax.ShapeDtypeStruct((depth, size, size), jnp.float32)
    f32 = jnp.float32
    dma = pltpu.SemaphoreType.DMA
    return pl.pallas_call(
        step_kernel,
        in_specs=[scalars, scalars] + [anywhere] * 5,
        out_specs=[anywhere, anywhere],
        out_shape=(slab, slab),
        scratch_shapes=[
            pltpu.VMEM(tables.shape, jnp.bfloat16),
            pltpu.VMEM((2, 2, planes, size, size), f32),
            pltpu.VMEM((bands, devices, depth, 2, planes, size), f32),
            pltpu.VMEM((bands, devices, depth, 2, planes, size), f32),
            pltpu.VMEM((points, depth, size, size), f32),
            pltpu.VMEM((hist, depth, size, size), f32),
            pltpu.VMEM((hist, depth, size, size), f32),
            pltpu.VMEM((depth, size, size), f32),
            pltpu.VMEM((2, depth, size, size), f32),
            pltpu.VMEM((1, 128), f32),
            pltpu.VMEM((points, 1, 128), f32),
            pltpu.VMEM((devices, 1, 128), f32),
            pltpu.VMEM((points * devices, 1, 128), f32),
            pltpu.VMEM((hist, 8, size), f32),
            pltpu.VMEM((hist + 8, 128), f32),
            dma((4,)), dma((2,)),
            dma((bands - 1 + pairs,)), dma((bands - 1 + pairs,)),
            dma((3,)), dma((3,)), dma((pairs,)), dma((pairs,)), dma((2 * pairs,)),
        ],
        compiler_params=pltpu.CompilerParams(
            collective_id=0, has_side_effects=True, vmem_limit_bytes=56 * 1024 * 1024
        ),
    )(occupations, weights, tables, psi_hat, density_in, dens_hist, resid_hist)


def solution(mesh):
    return jax.shard_map(
        shards,
        mesh=mesh,
        in_specs=(
            P("ka", None, None, "band", None, None),
            P("ka", None),
            P("ka"),
            P("band", None, None),
            P(None, "band", None, None),
            P(None, "band", None, None),
        ),
        out_specs=(P("band", None, None), P("band", None, None)),
        check_vma=False,
    )
```

```python
from functools import partial

import jax
import jax.numpy as jnp
import numpy as np
from jax import lax
from jax.experimental import pallas as pl
from jax.experimental.pallas import tpu as pltpu
from jax.sharding import PartitionSpec as P

beta_mix = 0.3
regular = 0.01
LAG = 3
LAST = 2
MESH = pl.DeviceIdType.MESH


def rotation_tables(size):
    indices = np.arange(size)
    angles = (indices[:, None] * indices[None, :] % size) * (2.0 * np.pi / size)
    cosine, sine = np.cos(angles), np.sin(angles)
    table = np.block([[cosine, sine], [-sine, cosine]]).astype(np.float32)
    high = table.astype(jnp.bfloat16)
    low = (table - high.astype(np.float32)).astype(jnp.bfloat16)
    return np.stack([high, low, high.T, low.T])


def split(value):
    high = value.astype(jnp.bfloat16)
    return high, (value - high.astype(jnp.float32)).astype(jnp.bfloat16)


def dot3(left, right, contract):
    dims = (contract, ((), ()))
    dot = partial(lax.dot_general, dimension_numbers=dims, preferred_element_type=jnp.float32)
    return dot(left[0], right[0]) + (dot(left[0], right[1]) + dot(left[1], right[0]))


def partner(index, step, count):
    if count & (count - 1):
        return lax.rem(index + step, count)
    result, bit = index, 1
    while bit < count:
        if step & bit:
            result = result + bit * (1 - 2 * lax.rem(index // bit, 2))
        bit *= 2
    return result


def total(value):
    return jnp.sum(jnp.sum(value, axis=0, keepdims=True), axis=1, keepdims=True)


def step_kernel(
    scalar_ref, tables_hbm, psi_hbm, density_in_hbm, dens_hbm, resid_hbm,
    first_ref, others_ref, update_ref,
    tables, psi, send, recv, pools, resid, dens, density_in, share, wbuf, grams, lates,
    late_acc, inverse,
    in_sem, psi_sem, send_sem, recv_sem, small_send, small_recv, pool_send, pool_recv,
):
    points, devices = lax.axis_size("ka"), lax.axis_size("band")
    bands, _, depth, _, planes, size = send.shape[0], *send.shape[1:]
    hist = resid.shape[0]
    everyone = points * devices
    pairs, early = depth // 2, bands - LAST
    ka, me = lax.axis_index("ka"), lax.axis_index("band")
    flat = ka * devices + me
    half = devices // 2
    steps = [s for low in range(half - 1, -1, -1) for s in (half + low, low) if s]
    some_band = (ka, partner(me, 1, devices))
    some_point = (lax.rem(ka + 1, points), me)

    def remote(source, target, send_s, recv_s, device):
        return pltpu.make_async_remote_copy(
            src_ref=source, dst_ref=target, send_sem=send_s, recv_sem=recv_s,
            device_id=device, device_id_type=MESH,
        )

    def psi_copy(band, slot):
        return pltpu.make_async_copy(psi_hbm.at[0, band], psi.at[slot], psi_sem.at[slot])

    tables_copy = pltpu.make_async_copy(tables_hbm, tables, in_sem.at[0])
    resid_copy = pltpu.make_async_copy(resid_hbm, resid, in_sem.at[1])
    dens_copy = pltpu.make_async_copy(dens_hbm, dens, in_sem.at[2])
    base_copy = pltpu.make_async_copy(density_in_hbm, density_in, in_sem.at[3])

    psi_copy(0, 0).start()
    tables_copy.start()
    psi_copy(1, 1).start()
    barrier = pltpu.get_barrier_semaphore()

    def greet(step, carry):
        other = lax.rem(flat + step, everyone)
        pl.semaphore_signal(
            barrier, inc=1, device_id=(other // devices, lax.rem(other, devices)),
            device_id_type=MESH,
        )
        return carry

    lax.fori_loop(1, everyone, greet, 0)
    base_copy.start()
    resid_copy.start()
    dens_copy.start()
    pools[pl.ds(ka, 1)] = jnp.zeros((1, depth, size, size), jnp.float32)
    late_acc[...] = jnp.zeros(late_acc.shape, jnp.float32)
    wbuf[pl.ds(ka, 1)] = jnp.full((1, 1, 128), scalar_ref[0, bands])
    tables_copy.wait()

    def send_planes(cut):
        for s in steps:
            other = partner(me, s, devices)
            remote(
                send.at[0, other, :, :, cut], recv.at[0, me, :, :, cut],
                send_sem.at[0], recv_sem.at[0], (ka, other),
            ).start()

    def produce(band, slot):
        psi_copy(band, slot).wait()
        for p in range(planes):
            pair = jnp.concatenate([psi[slot, 0, p], psi[slot, 1, p]], axis=1)
            after_kz = dot3((tables[2], tables[3]), split(pair), ((1,), (1,)))
            rows = jnp.concatenate([after_kz[:size], after_kz[size:]], axis=1)
            after_ky = dot3(split(rows), (tables[0], tables[1]), ((1,), (0,)))
            for part in range(2):
                piece = after_ky[:, part * size : (part + 1) * size]
                send[band, :, :, part, p, :] = piece.reshape(devices, depth, size)
            if p == planes // 2 - 1:

                @pl.when(band == 0)
                def _():
                    pl.semaphore_wait(barrier, everyone - 1)
                    send_planes(pl.ds(0, planes // 2))

        recv[band, pl.ds(me, 1)] = send[band, pl.ds(me, 1)]

    def transform(band, layers):
        columns = []
        for z in layers:
            parts = [recv[band, :, z, c].reshape(devices * planes, size) for c in range(2)]
            columns.append(jnp.concatenate(parts, axis=0))
        field = dot3(
            (tables[2], tables[3]), split(jnp.concatenate(columns, axis=1)), ((1,), (0,))
        )
        power = field[:size] * field[:size] + field[size:] * field[size:]
        scale = share[...] * scalar_ref[0, band]
        for i, z in enumerate(layers):
            pools[ka, z] += scale * power[:, i * size : (i + 1) * size]

    def consume(band):
        remote(
            send.at[band, pl.ds(0, devices - 1)], recv.at[band, pl.ds(0, devices - 1)],
            send_sem.at[band], recv_sem.at[band], some_band,
        ).wait_recv()

        def body(pair, carry):
            transform(band, (2 * pair, 2 * pair + 1))
            return carry

        lax.fori_loop(0, pairs, body, 0)

    def send_weight():
        for step in range(1, points):
            remote(
                wbuf.at[ka], wbuf.at[ka], small_send.at[0], small_recv.at[0],
                (lax.rem(ka + step, points), me),
            ).start()

    def history():
        remote(
            wbuf.at[pl.ds(0, points - 1)], wbuf.at[pl.ds(0, points - 1)],
            small_send.at[0], small_recv.at[0], some_point,
        ).wait()
        weight_total = wbuf[0]
        for k in range(1, points):
            weight_total = weight_total + wbuf[k]
        share[...] = wbuf[ka] / weight_total * jnp.float32(1.0 / size**3)
        base_copy.wait()
        resid_copy.wait()
        dens_copy.wait()
        which = [(h, g) for h in range(hist) for g in range(h + 1)]
        blocks = size // 8

        def body(i, sums):
            z, x = i // blocks, pl.multiple_of(lax.rem(i, blocks) * 8, 8)
            rows = [resid[h, z, pl.ds(x, 8)] for h in range(hist)]
            start = density_in[z, pl.ds(x, 8)]
            for h in range(hist):
                dens[h, z, pl.ds(x, 8)] = dens[h, z, pl.ds(x, 8)] + beta_mix * rows[h]
            products = [rows[h] * rows[g] for h, g in which] + [row * start for row in rows]
            return tuple(s + p for s, p in zip(sums, products))

        zeros = tuple(jnp.zeros((8, size), jnp.float32) for _ in range(len(which) + hist))
        sums = lax.fori_loop(0, depth * blocks, body, zeros)
        lane = lax.broadcasted_iota(jnp.int32, (1, 128), 1)
        row = jnp.zeros((1, 128), jnp.float32)
        for (h, g), value in zip(which, sums):
            here = (lane == h * hist + g) | (lane == g * hist + h)
            row = jnp.where(here, total(value), row)
        for h in range(hist):
            row = jnp.where(lane == hist * hist + h, total(sums[len(which) + h]), row)
        grams[pl.ds(me, 1)] = row[None]
        for step in steps:
            remote(
                grams.at[me], grams.at[me], small_send.at[1], small_recv.at[1],
                (ka, partner(me, step, devices)),
            ).start()

    def factor():
        rest = pl.ds(0, devices - 1)
        remote(
            grams.at[rest], grams.at[rest], small_send.at[1], small_recv.at[1], some_band
        ).wait()
        row = grams[0]
        for d in range(1, devices):
            row = row + grams[d]
        lane = lax.broadcasted_iota(jnp.int32, (hist, 128), 1)
        level = lax.broadcasted_iota(jnp.int32, (hist, 128), 0)
        wide = jnp.broadcast_to(row, (hist, 128))
        start = jnp.zeros((1, 1), jnp.float32)
        gram = jnp.zeros((hist, 128), jnp.float32)
        for g in range(hist):
            picked = jnp.sum(
                jnp.where(lane == level * hist + g, wide, 0.0), axis=1, keepdims=True
            )
            gram = jnp.where(lane == g, picked, gram)
        first = jnp.sum(
            jnp.where(lane == hist * hist + level, wide, 0.0), axis=1, keepdims=True
        )
        start = jnp.sum(jnp.where(lane == level, first, 0.0), axis=0, keepdims=True)
        work = jnp.where(lane == level, gram + regular * gram, gram)
        right = jnp.where(lane == level, jnp.float32(1.0), 0.0)
        for j in range(hist):
            pivot = jnp.sum(
                jnp.where((lane == j) & (level == j), work, 0.0), axis=(0, 1), keepdims=True
            )
            root = jnp.sqrt(pivot)
            column = jnp.sum(jnp.where(lane == j, work, 0.0), axis=1, keepdims=True) / root
            line = jnp.sum(jnp.where(level == j, work, 0.0), axis=0, keepdims=True) / root
            solved = jnp.sum(jnp.where(level == j, right, 0.0), axis=0, keepdims=True) / root
            work = work - column * line
            right = jnp.where(
                level == j, solved, jnp.where(level > j, right - column * solved, right)
            )
        inverse[0:hist] = right
        inverse[hist : hist + 1] = start

    def step(band, carry):
        slot = lax.rem(band, 2)
        produce(band, slot)

        @pl.when(band == 0)
        def _():
            send_planes(pl.ds(planes // 2, planes // 2))
            send_weight()

        @pl.when((band > 0) & (band < early))
        def _():
            for s in steps:
                other = partner(me, s, devices)
                remote(
                    send.at[band, other], recv.at[band, me],
                    send_sem.at[band], recv_sem.at[band], (ka, other),
                ).start()

        @pl.when(band == bands - 1)
        def _():
            def layer(z, carry):
                for s in steps:
                    other = partner(me, s, devices)
                    tail = pl.ds(early, LAST)
                    remote(
                        send.at[tail, other, z], recv.at[tail, me, z],
                        send_sem.at[early + z], recv_sem.at[early + z], (ka, other),
                    ).start()
                return carry

            lax.fori_loop(0, depth, layer, 0)

        @pl.when(band + 2 < bands)
        def _():
            psi_copy(band + 2, slot).start()

        @pl.when(band == LAG - 1)
        def _():
            history()

        @pl.when(band >= LAG)
        def _():
            consume(band - LAG)

        return carry

    lax.fori_loop(0, bands, step, 0)
    factor()

    def drain(band, carry):
        consume(band)
        return carry

    lax.fori_loop(bands - LAG, early, drain, 0)

    def send_pool(z):
        for s in range(1, points):
            remote(
                pools.at[ka, z], pools.at[ka, z], pool_send.at[z], pool_recv.at[z],
                (lax.rem(ka + s, points), me),
            ).start()

    def gather(z):
        rest = pools.at[pl.ds(0, points - 1), z]
        remote(rest, rest, pool_send.at[z], pool_recv.at[z], some_point).wait()
        others = pools[1, z]
        for k in range(2, points):
            others = others + pools[k, z]
        first_ref[z] = pools[0, z]
        others_ref[z] = others

    def last_bands(z):
        return remote(
            send.at[pl.ds(early, LAST), pl.ds(0, devices - 1), z],
            recv.at[pl.ds(early, LAST), pl.ds(0, devices - 1), z],
            send_sem.at[early + z], recv_sem.at[early + z], some_band,
        )

    def finish(z):
        last_bands(z).wait_recv()
        for band in range(early, bands):
            transform(band, (z,))

    def project(z):
        for h in range(hist):
            product = resid[h, z] * pools[ka, z]
            late_acc[h] += jnp.sum(product.reshape(size // 8, 8, size), axis=0)

    def layer(z, carry):
        finish(z)
        project(z)
        send_pool(z)

        @pl.when(z > 0)
        def _():
            gather(z - 1)

        return carry

    lax.fori_loop(0, depth - 1, layer, 0)
    finish(depth - 1)
    project(depth - 1)
    lane = lax.broadcasted_iota(jnp.int32, (hist, 128), 1)
    level = lax.broadcasted_iota(jnp.int32, (hist, 128), 0)
    sums = jnp.sum(jnp.sum(late_acc[...], axis=1), axis=1, keepdims=True)
    row = jnp.sum(jnp.where(lane == level, sums, 0.0), axis=0, keepdims=True)
    lates[pl.ds(flat, 1)] = row[None]

    def tell(step, carry):
        other = lax.rem(flat + step, everyone)
        remote(
            lates.at[flat], lates.at[flat], small_send.at[2], small_recv.at[2],
            (other // devices, lax.rem(other, devices)),
        ).start()
        return carry

    lax.fori_loop(1, everyone, tell, 0)
    send_pool(depth - 1)
    if depth > 1:
        gather(depth - 2)
    gather(depth - 1)
    rest = lates.at[pl.ds(0, everyone - 1)]
    remote(rest, rest, small_send.at[2], small_recv.at[2], some_band).wait()
    late = lates[0]
    for d in range(1, everyone):
        late = late + lates[d]
    factor_inverse = inverse[0:hist]
    halfway = jnp.sum(
        factor_inverse * (late - inverse[hist : hist + 1]), axis=1, keepdims=True
    )
    coefs = jnp.sum(factor_inverse * halfway, axis=0, keepdims=True)
    coefs = [
        jnp.sum(jnp.where(lane[:1] == h, coefs, 0.0), axis=1, keepdims=True) for h in range(hist)
    ]
    for z in range(depth):
        update = coefs[0] * dens[0, z]
        for h in range(1, hist):
            update = update + coefs[h] * dens[h, z]
        update_ref[z] = update

    rest = pl.ds(0, devices - 1)

    def sent(band, carry):
        remote(
            send.at[band, rest], recv.at[band, rest], send_sem.at[band], recv_sem.at[band],
            some_band,
        ).wait_send()
        return carry

    lax.fori_loop(0, early, sent, 0)

    def last_sent(z, carry):
        last_bands(z).wait_send()
        return carry

    lax.fori_loop(0, depth, last_sent, 0)


def shards(psi_hat, occupations, weights, density_in, dens_hist, resid_hist):
    devices, points = lax.axis_size("band"), lax.axis_size("ka")
    _, bands, _, planes, size, _ = psi_hat.shape
    hist = resid_hist.shape[0]
    depth = size // devices
    tables = jnp.asarray(rotation_tables(size))
    anywhere = pl.BlockSpec(memory_space=pltpu.HBM)
    scalars = pl.BlockSpec(memory_space=pltpu.SMEM)
    numbers = jnp.concatenate([occupations[0], weights]).astype(jnp.float32)[None]
    resident = pl.BlockSpec(memory_space=pltpu.VMEM)
    slab = jax.ShapeDtypeStruct((depth, size, size), jnp.float32)
    f32 = jnp.float32
    dma = pltpu.SemaphoreType.DMA
    first, others, update = pl.pallas_call(
        step_kernel,
        in_specs=[scalars] + [anywhere] * 5,
        out_specs=[resident] * 3,
        out_shape=(slab, slab, slab),
        scratch_shapes=[
            pltpu.VMEM(tables.shape, jnp.bfloat16),
            pltpu.VMEM((2, 2, planes, size, size), f32),
            pltpu.VMEM((bands, devices, depth, 2, planes, size), f32),
            pltpu.VMEM((bands, devices, depth, 2, planes, size), f32),
            pltpu.VMEM((points, depth, size, size), f32),
            pltpu.VMEM((hist, depth, size, size), f32),
            pltpu.VMEM((hist, depth, size, size), f32),
            pltpu.VMEM((depth, size, size), f32),
            pltpu.VMEM((1, 128), f32),
            pltpu.VMEM((points, 1, 128), f32),
            pltpu.VMEM((devices, 1, 128), f32),
            pltpu.VMEM((points * devices, 1, 128), f32),
            pltpu.VMEM((hist, 8, size), f32),
            pltpu.VMEM((hist + 8, 128), f32),
            dma((4,)), dma((2,)),
            dma((bands - LAST + depth,)), dma((bands - LAST + depth,)),
            dma((3,)), dma((3,)), dma((depth,)), dma((depth,)),
        ],
        compiler_params=pltpu.CompilerParams(
            collective_id=0, has_side_effects=True, vmem_limit_bytes=52 * 1024 * 1024
        ),
    )(numbers, tables, psi_hat, density_in, dens_hist, resid_hist)
    density = first + others
    return density, density_in + beta_mix * (density - density_in) - update


def solution(mesh):
    return jax.shard_map(
        shards,
        mesh=mesh,
        in_specs=(
            P("ka", None, None, "band", None, None),
            P("ka", None),
            P("ka"),
            P("band", None, None),
            P(None, "band", None, None),
            P(None, "band", None, None),
        ),
        out_specs=(P("band", None, None), P("band", None, None)),
        check_vma=False,
    )
```

```python
from functools import partial

import jax
import jax.numpy as jnp
import numpy as np
from jax import lax
from jax.experimental import pallas as pl
from jax.experimental.pallas import tpu as pltpu
from jax.sharding import PartitionSpec as P

beta_mix = 0.3
regular = 0.01
LAG = 3
LAST = 3
MESH = pl.DeviceIdType.MESH


def rotation_tables(size):
    indices = np.arange(size)
    angles = (indices[:, None] * indices[None, :] % size) * (2.0 * np.pi / size)
    cosine, sine = np.cos(angles), np.sin(angles)
    table = np.block([[cosine, sine], [-sine, cosine]]).astype(np.float32)
    high = table.astype(jnp.bfloat16)
    low = (table - high.astype(np.float32)).astype(jnp.bfloat16)
    return np.stack([high, low, high.T, low.T])


def split(value):
    high = value.astype(jnp.bfloat16)
    return high, (value - high.astype(jnp.float32)).astype(jnp.bfloat16)


def dot3(left, right, contract):
    dims = (contract, ((), ()))
    dot = partial(lax.dot_general, dimension_numbers=dims, preferred_element_type=jnp.float32)
    return dot(left[0], right[0]) + (dot(left[0], right[1]) + dot(left[1], right[0]))


def partner(index, step, count):
    if count & (count - 1):
        return lax.rem(index + step, count)
    result, bit = index, 1
    while bit < count:
        if step & bit:
            result = result + bit * (1 - 2 * lax.rem(index // bit, 2))
        bit *= 2
    return result


def total(value):
    return jnp.sum(jnp.sum(value, axis=0, keepdims=True), axis=1, keepdims=True)


def step_kernel(
    occ_hbm, weight_hbm, tables_hbm, psi_hbm, density_in_hbm, dens_hbm, resid_hbm,
    first_ref, others_ref, update_ref,
    tables, psi, send, recv, pools, resid, dens, density_in, share, wbuf, grams, lates,
    late_acc, inverse, occ_ref, weight_ref,
    in_sem, psi_sem, send_sem, recv_sem, small_send, small_recv, pool_send, pool_recv,
):
    points, devices = lax.axis_size("ka"), lax.axis_size("band")
    bands, _, depth, _, planes, size = send.shape[0], *send.shape[1:]
    hist = resid.shape[0]
    everyone = points * devices
    pairs, early = depth // 2, bands - LAST
    ka, me = lax.axis_index("ka"), lax.axis_index("band")
    flat = ka * devices + me
    half = devices // 2
    steps = [s for low in range(half - 1, -1, -1) for s in (half + low, low) if s]
    nearby = [partner(me, s, devices) for s in range(half - 1, 0, -1)]
    if devices % 4:
        far = [partner(me, s, devices) for s in range(devices - 1, half - 1, -1)]
    else:
        quarter = devices // 4
        side, within = me // half, lax.rem(me, quarter)
        far = [
            ((1 - side) * k + side * (3 - k)) * quarter + partner(within, s, quarter)
            for k in (3, 2) for s in range(quarter)
        ]
    outer = [other for pair in zip(far, nearby) for other in pair] + far[len(nearby) :]
    others = [
        (lax.rem(ka + k, points), partner(me, s, devices))
        for s in range(devices - 1, -1, -1) for k in range(points - 1, -1, -1) if s or k
    ]
    some_band = (ka, partner(me, 1, devices))
    some_point = (lax.rem(ka + 1, points), me)

    def remote(source, target, send_s, recv_s, device):
        return pltpu.make_async_remote_copy(
            src_ref=source, dst_ref=target, send_sem=send_s, recv_sem=recv_s,
            device_id=device, device_id_type=MESH,
        )

    def psi_copy(band, slot):
        return pltpu.make_async_copy(psi_hbm.at[0, band], psi.at[slot], psi_sem.at[slot])

    tables_copy = pltpu.make_async_copy(tables_hbm, tables, in_sem.at[0])
    resid_copy = pltpu.make_async_copy(resid_hbm, resid, in_sem.at[1])
    dens_copy = pltpu.make_async_copy(dens_hbm, dens, in_sem.at[2])
    base_copy = pltpu.make_async_copy(density_in_hbm, density_in, in_sem.at[3])

    psi_copy(0, 0).start()
    tables_copy.start()
    pltpu.make_async_copy(occ_hbm, occ_ref, in_sem.at[4]).start()
    pltpu.make_async_copy(weight_hbm, weight_ref, in_sem.at[5]).start()
    psi_copy(1, 1).start()
    barrier = pltpu.get_barrier_semaphore()

    for device in others:
        pl.semaphore_signal(barrier, inc=1, device_id=device, device_id_type=MESH)
    base_copy.start()
    resid_copy.start()
    dens_copy.start()
    pools[pl.ds(ka, 1)] = jnp.zeros((1, depth, size, size), jnp.float32)
    late_acc[...] = jnp.zeros(late_acc.shape, jnp.float32)
    pltpu.make_async_copy(occ_hbm, occ_ref, in_sem.at[4]).wait()
    pltpu.make_async_copy(weight_hbm, weight_ref, in_sem.at[5]).wait()
    wbuf[pl.ds(ka, 1)] = jnp.full((1, 1, size), weight_ref[0].astype(jnp.float32))
    tables_copy.wait()

    def send_planes(cut):
        for s in steps:
            other = partner(me, s, devices)
            remote(
                send.at[0, other, :, :, cut], recv.at[0, me, :, :, cut],
                send_sem.at[0], recv_sem.at[0], (ka, other),
            ).start()

    def produce(band, slot):
        psi_copy(band, slot).wait()
        for p in range(planes):
            pair = jnp.concatenate([psi[slot, 0, p], psi[slot, 1, p]], axis=1)
            after_kz = dot3((tables[2], tables[3]), split(pair), ((1,), (1,)))
            rows = jnp.concatenate([after_kz[:size], after_kz[size:]], axis=1)
            after_ky = dot3(split(rows), (tables[0], tables[1]), ((1,), (0,)))
            for part in range(2):
                piece = after_ky[:, part * size : (part + 1) * size]
                send[band, :, :, part, p, :] = piece.reshape(devices, depth, size)
            if p == planes // 2 - 1:

                @pl.when(band == 0)
                def _():
                    pl.semaphore_wait(barrier, everyone - 1)
                    send_planes(pl.ds(0, planes // 2))

        recv[band, pl.ds(me, 1)] = send[band, pl.ds(me, 1)]

    def transform(pieces):
        columns = []
        for band, z in pieces:
            parts = [recv[band, :, z, c].reshape(devices * planes, size) for c in range(2)]
            columns.append(jnp.concatenate(parts, axis=0))
        field = dot3(
            (tables[2], tables[3]), split(jnp.concatenate(columns, axis=1)), ((1,), (0,))
        )
        power = field[:size] * field[:size] + field[size:] * field[size:]
        for i, (band, z) in enumerate(pieces):
            scale = share[...] * occ_ref[0, band].astype(jnp.float32)
            pools[ka, z] += scale * power[:, i * size : (i + 1) * size]

    def consume(band):
        remote(
            send.at[band, pl.ds(0, devices - 1)], recv.at[band, pl.ds(0, devices - 1)],
            send_sem.at[band], recv_sem.at[band], some_band,
        ).wait_recv()

        def body(pair, carry):
            transform([(band, 2 * pair), (band, 2 * pair + 1)])
            return carry

        lax.fori_loop(0, pairs, body, 0)

    def send_weight():
        for step in range(1, points):
            remote(
                wbuf.at[ka], wbuf.at[ka], small_send.at[0], small_recv.at[0],
                (lax.rem(ka + step, points), me),
            ).start()

    def history():
        remote(
            wbuf.at[pl.ds(0, points - 1)], wbuf.at[pl.ds(0, points - 1)],
            small_send.at[0], small_recv.at[0], some_point,
        ).wait()
        weight_total = wbuf[0]
        for k in range(1, points):
            weight_total = weight_total + wbuf[k]
        share[...] = wbuf[ka] / weight_total * jnp.float32(1.0 / size**3)
        base_copy.wait()
        resid_copy.wait()
        dens_copy.wait()
        which = [(h, g) for h in range(hist) for g in range(h + 1)]
        blocks = size // 8

        def body(i, sums):
            z, x = i // blocks, pl.multiple_of(lax.rem(i, blocks) * 8, 8)
            rows = [resid[h, z, pl.ds(x, 8)] for h in range(hist)]
            start = density_in[z, pl.ds(x, 8)]
            for h in range(hist):
                dens[h, z, pl.ds(x, 8)] = dens[h, z, pl.ds(x, 8)] + beta_mix * rows[h]
            products = [rows[h] * rows[g] for h, g in which] + [row * start for row in rows]
            return tuple(s + p for s, p in zip(sums, products))

        zeros = tuple(jnp.zeros((8, size), jnp.float32) for _ in range(len(which) + hist))
        sums = lax.fori_loop(0, depth * blocks, body, zeros)
        lane = lax.broadcasted_iota(jnp.int32, (1, 128), 1)
        row = jnp.zeros((1, 128), jnp.float32)
        for (h, g), value in zip(which, sums):
            here = (lane == h * hist + g) | (lane == g * hist + h)
            row = jnp.where(here, total(value), row)
        for h in range(hist):
            row = jnp.where(lane == hist * hist + h, total(sums[len(which) + h]), row)
        grams[pl.ds(me, 1)] = row[None]
        for step in steps:
            remote(
                grams.at[me], grams.at[me], small_send.at[1], small_recv.at[1],
                (ka, partner(me, step, devices)),
            ).start()

    def factor():
        rest = pl.ds(0, devices - 1)
        remote(
            grams.at[rest], grams.at[rest], small_send.at[1], small_recv.at[1], some_band
        ).wait()
        row = grams[0]
        for d in range(1, devices):
            row = row + grams[d]
        lane = lax.broadcasted_iota(jnp.int32, (hist, 128), 1)
        level = lax.broadcasted_iota(jnp.int32, (hist, 128), 0)
        wide = jnp.broadcast_to(row, (hist, 128))
        start = jnp.zeros((1, 1), jnp.float32)
        gram = jnp.zeros((hist, 128), jnp.float32)
        for g in range(hist):
            picked = jnp.sum(
                jnp.where(lane == level * hist + g, wide, 0.0), axis=1, keepdims=True
            )
            gram = jnp.where(lane == g, picked, gram)
        first = jnp.sum(
            jnp.where(lane == hist * hist + level, wide, 0.0), axis=1, keepdims=True
        )
        start = jnp.sum(jnp.where(lane == level, first, 0.0), axis=0, keepdims=True)
        work = jnp.where(lane == level, gram + regular * gram, gram)
        right = jnp.where(lane == level, jnp.float32(1.0), 0.0)
        for j in range(hist):
            pivot = jnp.sum(
                jnp.where((lane == j) & (level == j), work, 0.0), axis=(0, 1), keepdims=True
            )
            root = jnp.sqrt(pivot)
            column = jnp.sum(jnp.where(lane == j, work, 0.0), axis=1, keepdims=True) / root
            line = jnp.sum(jnp.where(level == j, work, 0.0), axis=0, keepdims=True) / root
            solved = jnp.sum(jnp.where(level == j, right, 0.0), axis=0, keepdims=True) / root
            work = work - column * line
            right = jnp.where(
                level == j, solved, jnp.where(level > j, right - column * solved, right)
            )
        squared = jnp.zeros((hist, 128), jnp.float32)
        for j in range(hist):
            line = jnp.sum(jnp.where(level == j, right, 0.0), axis=0, keepdims=True)
            column = jnp.sum(jnp.where(lane == level, line, 0.0), axis=1, keepdims=True)
            squared = squared + column * line
        inverse[0:hist] = squared
        inverse[hist : hist + 1] = start

    def step(band, carry):
        slot = lax.rem(band, 2)
        produce(band, slot)

        @pl.when(band == 0)
        def _():
            send_planes(pl.ds(planes // 2, planes // 2))
            send_weight()

        @pl.when((band > 0) & (band < early))
        def _():
            for s in steps:
                other = partner(me, s, devices)
                remote(
                    send.at[band, other], recv.at[band, me],
                    send_sem.at[band], recv_sem.at[band], (ka, other),
                ).start()

        @pl.when(band == bands - 1)
        def _():
            def layer(z, carry):
                for other in outer:
                    tail = pl.ds(early, LAST)
                    remote(
                        send.at[tail, other, z], recv.at[tail, me, z],
                        send_sem.at[early + z], recv_sem.at[early + z], (ka, other),
                    ).start()
                return carry

            lax.fori_loop(0, depth, layer, 0)

        @pl.when(band + 2 < bands)
        def _():
            psi_copy(band + 2, slot).start()

        @pl.when(band == LAG - 1)
        def _():
            history()

        @pl.when(band >= LAG)
        def _():
            consume(band - LAG)

        return carry

    lax.fori_loop(0, bands, step, 0)
    factor()

    def drain(band, carry):
        consume(band)
        return carry

    lax.fori_loop(bands - LAG, early, drain, 0)

    def send_pool(z):
        for s in range(1, points):
            remote(
                pools.at[ka, z], pools.at[ka, z], pool_send.at[z], pool_recv.at[z],
                (lax.rem(ka + s, points), me),
            ).start()

    def gather(z):
        rest = pools.at[pl.ds(0, points - 1), z]
        remote(rest, rest, pool_send.at[z], pool_recv.at[z], some_point).wait()
        others = pools[1, z]
        for k in range(2, points):
            others = others + pools[k, z]
        first_ref[z] = pools[0, z]
        others_ref[z] = others

    def last_bands(z):
        return remote(
            send.at[pl.ds(early, LAST), pl.ds(0, devices - 1), z],
            recv.at[pl.ds(early, LAST), pl.ds(0, devices - 1), z],
            send_sem.at[early + z], recv_sem.at[early + z], some_band,
        )

    def finish(z):
        last_bands(z).wait_recv()
        transform([(band, z) for band in range(early, bands)])

    def project(z):
        for h in range(hist):
            product = resid[h, z] * pools[ka, z]
            late_acc[h] += jnp.sum(product.reshape(size // 8, 8, size), axis=0)

    def layer(z, carry):
        finish(z)
        project(z)
        send_pool(z)

        @pl.when(z > 0)
        def _():
            gather(z - 1)

        return carry

    lax.fori_loop(0, depth - 1, layer, 0)
    finish(depth - 1)
    project(depth - 1)
    lane = lax.broadcasted_iota(jnp.int32, (hist, 128), 1)
    level = lax.broadcasted_iota(jnp.int32, (hist, 128), 0)
    sums = jnp.sum(jnp.sum(late_acc[...], axis=1), axis=1, keepdims=True)
    row = jnp.sum(jnp.where(lane == level, sums, 0.0), axis=0, keepdims=True)
    lates[pl.ds(flat, 1)] = row[None]

    for device in others:
        remote(
            lates.at[flat], lates.at[flat], small_send.at[2], small_recv.at[2], device
        ).start()
    send_pool(depth - 1)
    if depth > 1:
        gather(depth - 2)
    gather(depth - 1)
    rest = lates.at[pl.ds(0, everyone - 1)]
    remote(rest, rest, small_send.at[2], small_recv.at[2], some_band).wait()
    late = lates[0]
    for d in range(1, everyone):
        late = late + lates[d]
    coefs = jnp.sum(inverse[0:hist] * (late - inverse[hist : hist + 1]), axis=1, keepdims=True)
    coefs = [coefs[h : h + 1] for h in range(hist)]
    for z in range(depth):
        update = coefs[0] * dens[0, z]
        for h in range(1, hist):
            update = update + coefs[h] * dens[h, z]
        update_ref[z] = update

    rest = pl.ds(0, devices - 1)

    def sent(band, carry):
        remote(
            send.at[band, rest], recv.at[band, rest], send_sem.at[band], recv_sem.at[band],
            some_band,
        ).wait_send()
        return carry

    lax.fori_loop(0, early, sent, 0)

    def last_sent(z, carry):
        last_bands(z).wait_send()
        return carry

    lax.fori_loop(0, depth, last_sent, 0)


def shards(psi_hat, occupations, weights, density_in, dens_hist, resid_hist):
    devices, points = lax.axis_size("band"), lax.axis_size("ka")
    _, bands, _, planes, size, _ = psi_hat.shape
    hist = resid_hist.shape[0]
    depth = size // devices
    tables = jnp.asarray(rotation_tables(size))
    anywhere = pl.BlockSpec(memory_space=pltpu.HBM)
    scalars = pl.BlockSpec(memory_space=pltpu.SMEM)
    resident = pl.BlockSpec(memory_space=pltpu.VMEM)
    slab = jax.ShapeDtypeStruct((depth, size, size), jnp.float32)
    f32 = jnp.float32
    dma = pltpu.SemaphoreType.DMA
    first, others, update = pl.pallas_call(
        step_kernel,
        in_specs=[anywhere] * 7,
        out_specs=[resident] * 3,
        out_shape=(slab, slab, slab),
        scratch_shapes=[
            pltpu.VMEM(tables.shape, jnp.bfloat16),
            pltpu.VMEM((2, 2, planes, size, size), f32),
            pltpu.VMEM((bands, devices, depth, 2, planes, size), f32),
            pltpu.VMEM((bands, devices, depth, 2, planes, size), f32),
            pltpu.VMEM((points, depth, size, size), f32),
            pltpu.VMEM((hist, depth, size, size), f32),
            pltpu.VMEM((hist, depth, size, size), f32),
            pltpu.VMEM((depth, size, size), f32),
            pltpu.VMEM((1, size), f32),
            pltpu.VMEM((points, 1, size), f32),
            pltpu.VMEM((devices, 1, 128), f32),
            pltpu.VMEM((points * devices, 1, 128), f32),
            pltpu.VMEM((hist, 8, size), f32),
            pltpu.VMEM((hist + 8, 128), f32),
            pltpu.SMEM((1, bands), jnp.int32), pltpu.SMEM((1,), jnp.int32),
            dma((6,)), dma((2,)),
            dma((bands - LAST + depth,)), dma((bands - LAST + depth,)),
            dma((3,)), dma((3,)), dma((depth,)), dma((depth,)),
        ],
        compiler_params=pltpu.CompilerParams(
            collective_id=0, has_side_effects=True, vmem_limit_bytes=52 * 1024 * 1024
        ),
    )(occupations, weights, tables, psi_hat, density_in, dens_hist, resid_hist)
    density = first + others
    return density, density_in + beta_mix * (density - density_in) - update


def solution(mesh):
    return jax.shard_map(
        shards,
        mesh=mesh,
        in_specs=(
            P("ka", None, None, "band", None, None),
            P("ka", None),
            P("ka"),
            P("band", None, None),
            P(None, "band", None, None),
            P(None, "band", None, None),
        ),
        out_specs=(P("band", None, None), P("band", None, None)),
        check_vma=False,
    )
```

```python
from functools import partial

import jax
import jax.numpy as jnp
import numpy as np
from jax import lax
from jax.experimental import pallas as pl
from jax.experimental.pallas import tpu as pltpu
from jax.sharding import PartitionSpec as P

beta_mix = 0.3
regular = 0.01
LAG = 3
LAST = 3
MESH = pl.DeviceIdType.MESH


def rotation_tables(size):
    indices = np.arange(size)
    angles = (indices[:, None] * indices[None, :] % size) * (2.0 * np.pi / size)
    cosine, sine = np.cos(angles), np.sin(angles)
    table = np.block([[cosine, sine], [-sine, cosine]]).astype(np.float32)
    high = table.astype(jnp.bfloat16)
    low = (table - high.astype(np.float32)).astype(jnp.bfloat16)
    return np.stack([high, low, high.T, low.T])


def split(value):
    high = value.astype(jnp.bfloat16)
    return high, (value - high.astype(jnp.float32)).astype(jnp.bfloat16)


def dot3(left, right, contract):
    dims = (contract, ((), ()))
    dot = partial(lax.dot_general, dimension_numbers=dims, preferred_element_type=jnp.float32)
    return dot(left[0], right[0]) + (dot(left[0], right[1]) + dot(left[1], right[0]))


def partner(index, step, count):
    if count & (count - 1):
        return lax.rem(index + step, count)
    result, bit = index, 1
    while bit < count:
        if step & bit:
            result = result + bit * (1 - 2 * lax.rem(index // bit, 2))
        bit *= 2
    return result


def total(value):
    return jnp.sum(jnp.sum(value, axis=0, keepdims=True), axis=1, keepdims=True)


def step_kernel(
    occ_hbm, weight_hbm, tables_hbm, psi_hbm, density_in_hbm, dens_hbm, resid_hbm,
    first_ref, others_ref, update_ref,
    tables, psi, send, recv, pools, resid, dens, density_in, share, wbuf, grams, lates,
    late_acc, inverse, occ_ref, weight_ref,
    in_sem, psi_sem, send_sem, recv_sem, small_send, small_recv, pool_send, pool_recv,
):
    points, devices = lax.axis_size("ka"), lax.axis_size("band")
    bands, _, depth, _, planes, size = send.shape[0], *send.shape[1:]
    hist = resid.shape[0]
    everyone = points * devices
    pairs, early = depth // 2, bands - LAST
    ka, me = lax.axis_index("ka"), lax.axis_index("band")
    flat = ka * devices + me
    half = devices // 2
    steps = [s for low in range(half - 1, -1, -1) for s in (half + low, low) if s]
    nearby = [partner(me, s, devices) for s in range(half - 1, 0, -1)]
    if devices % 4:
        far = [partner(me, s, devices) for s in range(devices - 1, half - 1, -1)]
    else:
        quarter = devices // 4
        side, within = me // half, lax.rem(me, quarter)
        far = [
            ((1 - side) * k + side * (3 - k)) * quarter + partner(within, s, quarter)
            for k in (3, 2) for s in range(quarter)
        ]
    outer = [other for pair in zip(far, nearby) for other in pair] + far[len(nearby) :]
    others = [
        (lax.rem(ka + k, points), partner(me, s, devices))
        for s in range(devices - 1, -1, -1) for k in range(points - 1, -1, -1) if s or k
    ]
    some_band = (ka, partner(me, 1, devices))
    some_point = (lax.rem(ka + 1, points), me)

    def remote(source, target, send_s, recv_s, device):
        return pltpu.make_async_remote_copy(
            src_ref=source, dst_ref=target, send_sem=send_s, recv_sem=recv_s,
            device_id=device, device_id_type=MESH,
        )

    def psi_copy(band, slot):
        return pltpu.make_async_copy(psi_hbm.at[0, band], psi.at[slot], psi_sem.at[slot])

    tables_copy = pltpu.make_async_copy(tables_hbm, tables, in_sem.at[0])
    resid_copy = pltpu.make_async_copy(resid_hbm, resid, in_sem.at[1])
    dens_copy = pltpu.make_async_copy(dens_hbm, dens, in_sem.at[2])
    base_copy = pltpu.make_async_copy(density_in_hbm, density_in, in_sem.at[3])

    psi_copy(0, 0).start()
    tables_copy.start()
    pltpu.make_async_copy(occ_hbm, occ_ref, in_sem.at[4]).start()
    pltpu.make_async_copy(weight_hbm, weight_ref, in_sem.at[5]).start()
    psi_copy(1, 1).start()
    barrier = pltpu.get_barrier_semaphore()

    for device in others:
        pl.semaphore_signal(barrier, inc=1, device_id=device, device_id_type=MESH)
    base_copy.start()
    resid_copy.start()
    dens_copy.start()
    pools[pl.ds(ka, 1)] = jnp.zeros((1, depth, size, size), jnp.float32)
    late_acc[...] = jnp.zeros(late_acc.shape, jnp.float32)
    pltpu.make_async_copy(occ_hbm, occ_ref, in_sem.at[4]).wait()
    pltpu.make_async_copy(weight_hbm, weight_ref, in_sem.at[5]).wait()
    wbuf[pl.ds(ka, 1)] = jnp.full((1, 1, size), weight_ref[0].astype(jnp.float32))
    tables_copy.wait()

    def send_planes(cut):
        for other in far + nearby:
            remote(
                send.at[0, other, :, :, cut], recv.at[0, me, :, :, cut],
                send_sem.at[0], recv_sem.at[0], (ka, other),
            ).start()

    def produce(band, slot):
        psi_copy(band, slot).wait()
        for p in range(planes):
            pair = jnp.concatenate([psi[slot, 0, p], psi[slot, 1, p]], axis=1)
            after_kz = dot3((tables[2], tables[3]), split(pair), ((1,), (1,)))
            rows = jnp.concatenate([after_kz[:size], after_kz[size:]], axis=1)
            after_ky = dot3(split(rows), (tables[0], tables[1]), ((1,), (0,)))
            for part in range(2):
                piece = after_ky[:, part * size : (part + 1) * size]
                send[band, :, :, part, p, :] = piece.reshape(devices, depth, size)
            if p == planes // 2 - 1:

                @pl.when(band == 0)
                def _():
                    pl.semaphore_wait(barrier, everyone - 1)
                    send_planes(pl.ds(0, planes // 2))

        recv[band, pl.ds(me, 1)] = send[band, pl.ds(me, 1)]

    def transform(pieces):
        columns = []
        for band, z in pieces:
            parts = [recv[band, :, z, c].reshape(devices * planes, size) for c in range(2)]
            columns.append(jnp.concatenate(parts, axis=0))
        field = dot3(
            (tables[2], tables[3]), split(jnp.concatenate(columns, axis=1)), ((1,), (0,))
        )
        power = field[:size] * field[:size] + field[size:] * field[size:]
        for i, (band, z) in enumerate(pieces):
            scale = share[...] * occ_ref[0, band].astype(jnp.float32)
            pools[ka, z] += scale * power[:, i * size : (i + 1) * size]

    def consume(band):
        remote(
            send.at[band, pl.ds(0, devices - 1)], recv.at[band, pl.ds(0, devices - 1)],
            send_sem.at[band], recv_sem.at[band], some_band,
        ).wait_recv()

        def body(pair, carry):
            transform([(band, 2 * pair), (band, 2 * pair + 1)])
            return carry

        lax.fori_loop(0, pairs, body, 0)

    def send_weight():
        for step in range(1, points):
            remote(
                wbuf.at[ka], wbuf.at[ka], small_send.at[0], small_recv.at[0],
                (lax.rem(ka + step, points), me),
            ).start()

    def history():
        remote(
            wbuf.at[pl.ds(0, points - 1)], wbuf.at[pl.ds(0, points - 1)],
            small_send.at[0], small_recv.at[0], some_point,
        ).wait()
        weight_total = wbuf[0]
        for k in range(1, points):
            weight_total = weight_total + wbuf[k]
        share[...] = wbuf[ka] / weight_total * jnp.float32(1.0 / size**3)
        base_copy.wait()
        resid_copy.wait()
        dens_copy.wait()
        which = [(h, g) for h in range(hist) for g in range(h + 1)]
        blocks = size // 8

        def body(i, sums):
            z, x = i // blocks, pl.multiple_of(lax.rem(i, blocks) * 8, 8)
            rows = [resid[h, z, pl.ds(x, 8)] for h in range(hist)]
            start = density_in[z, pl.ds(x, 8)]
            for h in range(hist):
                dens[h, z, pl.ds(x, 8)] = dens[h, z, pl.ds(x, 8)] + beta_mix * rows[h]
            products = [rows[h] * rows[g] for h, g in which] + [row * start for row in rows]
            return tuple(s + p for s, p in zip(sums, products))

        zeros = tuple(jnp.zeros((8, size), jnp.float32) for _ in range(len(which) + hist))
        sums = lax.fori_loop(0, depth * blocks, body, zeros)
        lane = lax.broadcasted_iota(jnp.int32, (1, 128), 1)
        row = jnp.zeros((1, 128), jnp.float32)
        for (h, g), value in zip(which, sums):
            here = (lane == h * hist + g) | (lane == g * hist + h)
            row = jnp.where(here, total(value), row)
        for h in range(hist):
            row = jnp.where(lane == hist * hist + h, total(sums[len(which) + h]), row)
        grams[pl.ds(me, 1)] = row[None]
        for step in steps:
            remote(
                grams.at[me], grams.at[me], small_send.at[1], small_recv.at[1],
                (ka, partner(me, step, devices)),
            ).start()

    def factor():
        rest = pl.ds(0, devices - 1)
        remote(
            grams.at[rest], grams.at[rest], small_send.at[1], small_recv.at[1], some_band
        ).wait()
        row = grams[0]
        for d in range(1, devices):
            row = row + grams[d]
        lane = lax.broadcasted_iota(jnp.int32, (hist, 128), 1)
        level = lax.broadcasted_iota(jnp.int32, (hist, 128), 0)
        wide = jnp.broadcast_to(row, (hist, 128))
        start = jnp.zeros((1, 1), jnp.float32)
        gram = jnp.zeros((hist, 128), jnp.float32)
        for g in range(hist):
            picked = jnp.sum(
                jnp.where(lane == level * hist + g, wide, 0.0), axis=1, keepdims=True
            )
            gram = jnp.where(lane == g, picked, gram)
        first = jnp.sum(
            jnp.where(lane == hist * hist + level, wide, 0.0), axis=1, keepdims=True
        )
        start = jnp.sum(jnp.where(lane == level, first, 0.0), axis=0, keepdims=True)
        work = jnp.where(lane == level, gram + regular * gram, gram)
        right = jnp.where(lane == level, jnp.float32(1.0), 0.0)
        for j in range(hist):
            pivot = jnp.sum(
                jnp.where((lane == j) & (level == j), work, 0.0), axis=(0, 1), keepdims=True
            )
            root = jnp.sqrt(pivot)
            column = jnp.sum(jnp.where(lane == j, work, 0.0), axis=1, keepdims=True) / root
            line = jnp.sum(jnp.where(level == j, work, 0.0), axis=0, keepdims=True) / root
            solved = jnp.sum(jnp.where(level == j, right, 0.0), axis=0, keepdims=True) / root
            work = work - column * line
            right = jnp.where(
                level == j, solved, jnp.where(level > j, right - column * solved, right)
            )
        squared = jnp.zeros((hist, 128), jnp.float32)
        for j in range(hist):
            line = jnp.sum(jnp.where(level == j, right, 0.0), axis=0, keepdims=True)
            column = jnp.sum(jnp.where(lane == level, line, 0.0), axis=1, keepdims=True)
            squared = squared + column * line
        inverse[0:hist] = squared
        inverse[hist : hist + 1] = start

    def step(band, carry):
        slot = lax.rem(band, 2)
        produce(band, slot)

        @pl.when(band == 0)
        def _():
            send_planes(pl.ds(planes // 2, planes // 2))
            send_weight()

        @pl.when((band > 0) & (band < early))
        def _():
            for other in outer:
                remote(
                    send.at[band, other], recv.at[band, me],
                    send_sem.at[band], recv_sem.at[band], (ka, other),
                ).start()

        @pl.when(band == bands - 1)
        def _():
            def layer(z, carry):
                for other in outer:
                    tail = pl.ds(early, LAST)
                    remote(
                        send.at[tail, other, z], recv.at[tail, me, z],
                        send_sem.at[early + z], recv_sem.at[early + z], (ka, other),
                    ).start()
                return carry

            lax.fori_loop(0, depth, layer, 0)

        @pl.when(band + 2 < bands)
        def _():
            psi_copy(band + 2, slot).start()

        @pl.when(band == LAG - 1)
        def _():
            history()

        @pl.when(band >= LAG)
        def _():
            consume(band - LAG)

        return carry

    lax.fori_loop(0, bands, step, 0)
    factor()

    def drain(band, carry):
        consume(band)
        return carry

    lax.fori_loop(bands - LAG, early, drain, 0)

    def send_pool(z):
        for s in range(1, points):
            remote(
                pools.at[ka, z], pools.at[ka, z], pool_send.at[z], pool_recv.at[z],
                (lax.rem(ka + s, points), me),
            ).start()

    def gather(z):
        rest = pools.at[pl.ds(0, points - 1), z]
        remote(rest, rest, pool_send.at[z], pool_recv.at[z], some_point).wait()
        others = pools[1, z]
        for k in range(2, points):
            others = others + pools[k, z]
        first_ref[z] = pools[0, z]
        others_ref[z] = others

    def last_bands(z):
        return remote(
            send.at[pl.ds(early, LAST), pl.ds(0, devices - 1), z],
            recv.at[pl.ds(early, LAST), pl.ds(0, devices - 1), z],
            send_sem.at[early + z], recv_sem.at[early + z], some_band,
        )

    def finish(z):
        last_bands(z).wait_recv()
        transform([(band, z) for band in range(early, bands)])

    def project(z):
        for h in range(hist):
            product = resid[h, z] * pools[ka, z]
            late_acc[h] += jnp.sum(product.reshape(size // 8, 8, size), axis=0)

    def layer(z, carry):
        finish(z)
        project(z)
        send_pool(z)

        @pl.when(z > 0)
        def _():
            gather(z - 1)

        return carry

    lax.fori_loop(0, depth - 1, layer, 0)
    finish(depth - 1)
    project(depth - 1)
    lane = lax.broadcasted_iota(jnp.int32, (hist, 128), 1)
    level = lax.broadcasted_iota(jnp.int32, (hist, 128), 0)
    sums = jnp.sum(jnp.sum(late_acc[...], axis=1), axis=1, keepdims=True)
    row = jnp.sum(jnp.where(lane == level, sums, 0.0), axis=0, keepdims=True)
    lates[pl.ds(flat, 1)] = row[None]

    for device in others:
        remote(
            lates.at[flat], lates.at[flat], small_send.at[2], small_recv.at[2], device
        ).start()
    send_pool(depth - 1)
    if depth > 1:
        gather(depth - 2)
    gather(depth - 1)
    rest = lates.at[pl.ds(0, everyone - 1)]
    remote(rest, rest, small_send.at[2], small_recv.at[2], some_band).wait()
    late = lates[0]
    for d in range(1, everyone):
        late = late + lates[d]
    coefs = jnp.sum(inverse[0:hist] * (late - inverse[hist : hist + 1]), axis=1, keepdims=True)
    coefs = [coefs[h : h + 1] for h in range(hist)]
    for z in range(depth):
        update = coefs[0] * dens[0, z]
        for h in range(1, hist):
            update = update + coefs[h] * dens[h, z]
        update_ref[z] = update

    rest = pl.ds(0, devices - 1)

    def sent(band, carry):
        remote(
            send.at[band, rest], recv.at[band, rest], send_sem.at[band], recv_sem.at[band],
            some_band,
        ).wait_send()
        return carry

    lax.fori_loop(0, early, sent, 0)

    def last_sent(z, carry):
        last_bands(z).wait_send()
        return carry

    lax.fori_loop(0, depth, last_sent, 0)


def shards(psi_hat, occupations, weights, density_in, dens_hist, resid_hist):
    devices, points = lax.axis_size("band"), lax.axis_size("ka")
    _, bands, _, planes, size, _ = psi_hat.shape
    hist = resid_hist.shape[0]
    depth = size // devices
    tables = jnp.asarray(rotation_tables(size))
    anywhere = pl.BlockSpec(memory_space=pltpu.HBM)
    scalars = pl.BlockSpec(memory_space=pltpu.SMEM)
    resident = pl.BlockSpec(memory_space=pltpu.VMEM)
    slab = jax.ShapeDtypeStruct((depth, size, size), jnp.float32)
    f32 = jnp.float32
    dma = pltpu.SemaphoreType.DMA
    first, others, update = pl.pallas_call(
        step_kernel,
        in_specs=[anywhere] * 7,
        out_specs=[resident] * 3,
        out_shape=(slab, slab, slab),
        scratch_shapes=[
            pltpu.VMEM(tables.shape, jnp.bfloat16),
            pltpu.VMEM((2, 2, planes, size, size), f32),
            pltpu.VMEM((bands, devices, depth, 2, planes, size), f32),
            pltpu.VMEM((bands, devices, depth, 2, planes, size), f32),
            pltpu.VMEM((points, depth, size, size), f32),
            pltpu.VMEM((hist, depth, size, size), f32),
            pltpu.VMEM((hist, depth, size, size), f32),
            pltpu.VMEM((depth, size, size), f32),
            pltpu.VMEM((1, size), f32),
            pltpu.VMEM((points, 1, size), f32),
            pltpu.VMEM((devices, 1, 128), f32),
            pltpu.VMEM((points * devices, 1, 128), f32),
            pltpu.VMEM((hist, 8, size), f32),
            pltpu.VMEM((hist + 8, 128), f32),
            pltpu.SMEM((1, bands), jnp.int32), pltpu.SMEM((1,), jnp.int32),
            dma((6,)), dma((2,)),
            dma((bands - LAST + depth,)), dma((bands - LAST + depth,)),
            dma((3,)), dma((3,)), dma((depth,)), dma((depth,)),
        ],
        compiler_params=pltpu.CompilerParams(
            collective_id=0, has_side_effects=True, vmem_limit_bytes=52 * 1024 * 1024
        ),
    )(occupations, weights, tables, psi_hat, density_in, dens_hist, resid_hist)
    density = first + others
    return density, density_in + beta_mix * (density - density_in) - update


def solution(mesh):
    return jax.shard_map(
        shards,
        mesh=mesh,
        in_specs=(
            P("ka", None, None, "band", None, None),
            P("ka", None),
            P("ka"),
            P("band", None, None),
            P(None, "band", None, None),
            P(None, "band", None, None),
        ),
        out_specs=(P("band", None, None), P("band", None, None)),
        check_vma=False,
    )
```
